32 devices in a mesh: gx: 4 (over y, x), gy: 8 (over z, core).
Axes of the slice: x: 2, y: 2, z: 4, core: 2. Of those that a mesh axis runs over, the one named last changes fastest.
Arguments:
- sources: bfloat16 [1024, 64, 512], P(('gx', 'gy')), may hold values from -6 to 6
- projection: bfloat16 [512, 512], replicated, may hold values from -0.25 to 0.25
- translations: bfloat16 [5, 2, 512, 512], replicated, may hold values from -0.1875 to 0.1875
- angles: float32 [6, 1024, 256], P(None, ('gx', 'gy')), may hold values from -3.140625 to 3.140625
- interpolation: bfloat16 [256, 1024], replicated, may hold values from -0.25 to 0.25
- box_order: int32 [1024], P(('gx', 'gy')), may hold values from 0 to 1023, as said below
Outputs:
- targets: bfloat16 [1024, 128, 512], P(('gx', 'gy'))
The draws below stay inside these ranges and needn't reach their ends.
Inputs may be any that keep to these rules, and one draw needn't show every extreme that they name: `box_order`: each aligned block of 32 entries (entries k * 32 to (k + 1) * 32 - 1) is a permutation of those same indices.
All inputs are finite; a program needn't handle non-finite values.
Results may differ from the reference program's by a relative error of at most 0.014.
Values may be sent and summed in bfloat16 or wider, within the bound.
A program may use at most 64 MiB of HBM per device.

```python
import jax
import jax.numpy as jnp
from jax import lax

K = 256
RHS = 64
POINTS = 512
BOX_DEV = 32
LEVELS = 5
BOXES = 1024
N_GX = 4
N_GY = 8


def draw_box_order(key, part):
    blocks = BOXES // BOX_DEV
    keys = jax.random.split(jax.random.fold_in(key, 17), blocks)
    orders = jax.vmap(lambda sub_key: jax.random.permutation(sub_key, BOX_DEV))(keys)
    offsets = jnp.arange(blocks, dtype=jnp.int32)[:, None] * BOX_DEV
    return (orders.astype(jnp.int32) + offsets).reshape(-1)


def levels(key, shape, cuts, least, high):
    gain = 1.0
    for dim, parts in cuts:
        draws = jax.random.uniform(jax.random.fold_in(jax.random.fold_in(key, 6), dim), (parts,), jnp.float32, least / len(cuts), high / len(cuts))
        gain = gain * jnp.repeat(jnp.exp(draws), shape[dim] // parts).reshape((-1,) + (1,) * (len(shape) - 1 - dim))
    return gain


def noise(key, shape, scale, bound, shards=(), kind=jnp.bfloat16):
    result = jax.random.normal(key, shape, jnp.float32) * scale
    if len(shards) > 0:
        result = levels(key, shape, shards, -0.22, 0.18) * result
    return jnp.clip(result, min=-bound, max=bound).astype(kind)


def setup_inputs(seed: int = 0) -> dict:
    splits = jax.random.split(jax.random.key(seed), 7)
    return {
        "sources": noise(splits[0], (BOXES, RHS, POINTS), 1.0, 6.0, ((0, 32),)),
        "projection": noise(splits[1], (POINTS, 2 * K), POINTS ** -0.5, 0.25),
        "translations": noise(splits[2], (LEVELS, 2, 2 * K, 2 * K), (4 * K) ** -0.5, 0.1875),
        "angles": jnp.clip(jax.random.uniform(splits[3], (LEVELS + 1, BOXES, K), jnp.float32, -3.140625, 3.140625), -3.140625, 3.140625),
        "interpolation": noise(splits[4], (K, 2 * POINTS), (2 * K) ** -0.5, 0.25),
        "box_order": draw_box_order(jax.random.fold_in(splits[6], 71), 0),
    }


def mix_parts(product, coeffs, sides):
    first_part = product[..., :coeffs]
    second_part = product[..., coeffs:]
    real_part = first_part[..., :sides, :] - second_part[..., sides:, :]
    imag_part = first_part[..., sides:, :] + second_part[..., :sides, :]
    return real_part, imag_part


def rotate(real_part, imag_part, angle_row):
    cosine = jnp.cos(angle_row)[..., None, :]
    sine_part = jnp.sin(angle_row)[..., None, :]
    return jnp.concatenate([cosine * real_part - sine_part * imag_part, sine_part * real_part + cosine * imag_part], axis=-2)


def level_plan(count_x, count_y):
    bits_x = count_x.bit_length() - 1
    bits_y = count_y.bit_length() - 1
    return [("gy", bits_y - 1), ("gx", bits_x - 1), ("gy", bits_y - 2), ("gx", bits_x - 2), ("gy", bits_y - 3)]


def interpolate(coeff_state, interpolation, sides, points):
    product = jnp.einsum("bck,kq->bcq", coeff_state.astype(jnp.float32), interpolation.astype(jnp.float32))
    real_part = product[:, :sides, :points] - product[:, sides:, points:]
    imag_part = product[:, :sides, points:] + product[:, sides:, :points]
    return jnp.concatenate([real_part, imag_part], axis=1).astype(jnp.bfloat16)


def reference(sources, projection, translations, angles, interpolation, box_order):
    devices = N_GX * N_GY

    def project(packed):
        source_block, order_block, angle_block = packed
        product = jnp.einsum("brp,pk->brk", source_block.astype(jnp.float32), projection.astype(jnp.float32))
        stacked = jnp.concatenate([product[..., :K], product[..., K:]], axis=1)
        placed = jnp.zeros_like(stacked).at[(order_block % BOX_DEV).astype(jnp.int32)].set(stacked)
        return rotate(placed[:, :RHS], placed[:, RHS:], angle_block).astype(jnp.bfloat16)

    coeff_state = lax.map(project, (sources.reshape(devices, BOX_DEV, RHS, POINTS), box_order.reshape(devices, BOX_DEV), angles[0].reshape(devices, BOX_DEV, K)))
    coeff_state = coeff_state.reshape(N_GX, N_GY, BOX_DEV, 2 * RHS, K)
    for level_no, (axis_name, bit_pos) in enumerate(level_plan(N_GX, N_GY)):
        dim_no = 0 if axis_name == "gx" else 1
        stride = 1 << bit_pos
        leading = jnp.moveaxis(coeff_state, dim_no, 0)
        extent = leading.shape[0]
        grouped = leading.reshape((extent // (2 * stride), 2, stride) + leading.shape[1:])
        angle_now = jnp.moveaxis(angles[level_no + 1].reshape(N_GX, N_GY, BOX_DEV, K), dim_no, 0)
        angle_now = angle_now.reshape((extent // (2 * stride), 2, stride) + angle_now.shape[1:])
        joined = jnp.concatenate([grouped[:, 0], grouped[:, 1]], axis=-1).astype(jnp.float32)
        halves = []
        for half_bit in range(2):
            product = jnp.einsum("...k,kq->...q", joined, translations[level_no, half_bit].astype(jnp.float32))
            real_part, imag_part = mix_parts(product, K, RHS)
            halves.append(rotate(real_part, imag_part, angle_now[:, half_bit]).astype(jnp.bfloat16))
        coeff_state = jnp.moveaxis(jnp.stack(halves, axis=1).reshape(leading.shape), 0, dim_no)
    per_peer = BOX_DEV // N_GY
    regrouped = coeff_state.reshape(N_GX, N_GY, N_GY, per_peer, 2 * RHS, K).transpose(0, 2, 1, 3, 4, 5)
    regrouped = regrouped.reshape(devices, BOX_DEV, 2 * RHS, K)
    targets = lax.map(lambda device_block: interpolate(device_block, interpolation, RHS, POINTS), regrouped)
    return targets.reshape(BOXES, 2 * RHS, POINTS)
```

```python
import functools

import jax
import jax.numpy as jnp
from jax import lax
from jax.experimental import pallas as pl
from jax.experimental.pallas import tpu as pltpu
from jax.sharding import PartitionSpec as P

SIDES = 8
SIN = (1.0, -0.16666666666602138, 0.00833333096559207, -0.00019840860009446372,
       2.752520673490089e-06, -2.3888051249402636e-08)
COS = (1.0, -0.4999999999699515, 0.04166666647185967, -0.001388888415088631,
       2.480103815897482e-05, -2.752459905052806e-07, 1.9906439107985886e-09)


def level_plan(count_x, count_y):
    bits_x = count_x.bit_length() - 1
    bits_y = count_y.bit_length() - 1
    return [
        ("gy", bits_y - 1),
        ("gx", bits_x - 1),
        ("gy", bits_y - 2),
        ("gx", bits_x - 2),
        ("gy", bits_y - 3),
    ]


def cos_sin(angle):
    half = angle * 0.5
    square = half * half

    def poly(coefs):
        total = jnp.full_like(square, coefs[-1])
        for coef in coefs[-2::-1]:
            total = total * square + coef
        return total

    sine, cosine = half * poly(SIN), poly(COS)
    return 1.0 - 2.0 * (sine * sine), 2.0 * (sine * cosine)


def kernel(
    count_x, count_y, sides,
    order_ref, angles_hbm, src_hbm, proj_hbm, w_hbm, interp_hbm,
    out_ref,
    ang, src, proj, w, interp, inverse, c0, s0, sent, got, ping, pong, back, home,
    phase_out, phase_in, last_out, last_in, cs, sn, cs_last, sn_last,
    load_sem, in_send, in_recv, out_send, out_recv, ang_send, ang_recv,
):
    f32, bf16 = jnp.float32, jnp.bfloat16
    nx, ny = 4, 8
    boxes = src.shape[0]
    coeffs = proj.shape[1] // 2
    points = interp.shape[1] // 2
    per_peer = boxes // count_y
    xl, yl = count_x // nx, count_y // ny
    simple = xl == 1 and yl == 1
    chunks = sides // SIDES
    lanes = ang.shape[2] // 2
    me_x, me_y = lax.axis_index("gx"), lax.axis_index("gy")
    group, group_low = me_x // xl, me_x % xl
    mine = group * ny + me_y // yl

    def spot(j, i):
        p = (me_y + j) % count_y
        r = (me_x + i) % per_peer
        return group_low + xl * (r * yl + me_y % yl), p, p * per_peer + r

    def origin(k, m):
        x = group_low + xl * ((group + k) % nx)
        return x, group % yl + yl * ((me_y // yl + m) % ny)

    def onto(k):
        return (group + k) % nx

    def remote(j, i, act):
        if j or i % per_peer:
            if simple or j:
                act()
                return
        elif simple:
            return
        pl.when(spot(j, i)[0] != me_x)(act)

    barrier = pltpu.get_barrier_semaphore()
    expected = 0
    for k in range(nx):
        for m in range(ny):
            if simple and not (k or m):
                continue
            x, y = origin(k, m)
            if simple:
                pl.semaphore_signal(
                    barrier, inc=1, device_id=(x, y), device_id_type=pl.DeviceIdType.MESH
                )
            else:
                @pl.when((x != me_x) | (y != me_y))
                def _(x=x, y=y):
                    pl.semaphore_signal(
                        barrier, inc=1, device_id=(x, y), device_id_type=pl.DeviceIdType.MESH
                    )
    if simple:
        expected = nx * ny - 1
    else:
        for k in range(1, nx):
            pl.semaphore_signal(
                barrier, inc=1, device_id=(group_low + xl * onto(k), me_y),
                device_id_type=pl.DeviceIdType.MESH,
            )
        for m in range(1, count_y):
            pl.semaphore_signal(
                barrier, inc=1, device_id=(me_x, (me_y + m) % count_y),
                device_id_type=pl.DeviceIdType.MESH,
            )
        own = (me_x // xl % yl == me_y % yl).astype(jnp.int32)
        expected = nx * ny - own + nx - 1 + count_y - 1

    pairs = chunks // 2
    loads = [
        pltpu.make_async_copy(angles_hbm, ang, load_sem.at[0]),
        pltpu.make_async_copy(proj_hbm, proj, load_sem.at[1]),
        pltpu.make_async_copy(interp_hbm, interp, load_sem.at[2]),
        pltpu.make_async_copy(w_hbm, w, load_sem.at[3]),
    ]
    pieces = pltpu.make_async_copy(src_hbm, src, load_sem.at[4])
    loads[0].start()
    loads[1].start()
    pieces.start()
    loads[3].start()
    loads[2].start()

    local = order_ref[...] % boxes
    place = lax.broadcasted_iota(jnp.int32, local.shape, 1)
    for slot in range(boxes):
        inverse[slot] = jnp.max(jnp.where(local == slot, place, 0))

    loads[0].wait()
    for first in range(0, boxes, 8):
        for level in range(4):
            for part in range(2):
                phase_out[pl.ds(first * 8 + level * 2 + part, 8, stride=8), :] = ang[
                    level + 1, first : first + 8, part * lanes : (part + 1) * lanes
                ]
    for slot in range(boxes):
        for part in range(2):
            row = slot // per_peer * 8 + slot % per_peer * 2 + part
            last_out[row : row + 1, :] = ang[5, slot : slot + 1, part * lanes : (part + 1) * lanes]
    cosine, sine = cos_sin(ang[0])
    c0[...] = cosine
    s0[...] = sine

    def turn(real, imag, cosine, sine):
        return jnp.concatenate(
            [cosine * real - sine * imag, sine * real + cosine * imag], axis=0
        ).astype(bf16)

    def project(cc):
        first = pl.multiple_of(cc * 2 * SIDES, 2 * SIDES)
        for half in range(2):
            slots = range(half * boxes // 2, (half + 1) * boxes // 2)
            rows = jnp.concatenate(
                [src[inverse[slot], pl.ds(first, 2 * SIDES), :] for slot in slots], axis=0
            )
            prod = jnp.dot(rows, proj[...], preferred_element_type=f32)
            for index, slot in enumerate(slots):
                for part in range(2):
                    at = (index * 2 + part) * SIDES
                    block = prod[at : at + SIDES]
                    sent[cc * 2 + part, slot] = turn(
                        block[:, :coeffs], block[:, coeffs:],
                        c0[slot : slot + 1, :], s0[slot : slot + 1, :],
                    )

    def in_copy(c, j, i):
        x, y, slot = spot(j, i)
        return pltpu.make_async_remote_copy(
            src_ref=sent.at[c, slot], dst_ref=got.at[c, mine],
            send_sem=in_send.at[c], recv_sem=in_recv.at[c],
            device_id=(x, y), device_id_type=pl.DeviceIdType.MESH,
        )

    def phase_copy(j, i):
        x, y, slot = spot(j, i)
        return pltpu.make_async_remote_copy(
            src_ref=phase_out.at[pl.ds(pl.multiple_of(slot * 8, 8), 8), :],
            dst_ref=phase_in.at[pl.ds(pl.multiple_of(mine * 8, 8), 8), :],
            send_sem=ang_send.at[0], recv_sem=ang_recv.at[0],
            device_id=(x, y), device_id_type=pl.DeviceIdType.MESH,
        )

    def last_copy(j):
        p = (me_y + j) % count_y
        return pltpu.make_async_remote_copy(
            src_ref=last_out.at[pl.ds(pl.multiple_of(p * 8, 8), 8), :],
            dst_ref=last_in.at[pl.ds(pl.multiple_of(me_y * 8, 8), 8), :],
            send_sem=ang_send.at[1], recv_sem=ang_recv.at[1],
            device_id=(me_x, p), device_id_type=pl.DeviceIdType.MESH,
        )

    def out_copy(c, k):
        return pltpu.make_async_remote_copy(
            src_ref=back.at[c, onto(k)], dst_ref=home.at[c, group],
            send_sem=out_send.at[c], recv_sem=out_recv.at[c],
            device_id=(group_low + xl * onto(k), me_y), device_id_type=pl.DeviceIdType.MESH,
        )

    far = sorted(range(count_y), key=lambda j: -min(j, count_y - j))
    blocks = [(j, i) for j in far for i in range(per_peer)]

    def keep(copy_own):
        if simple:
            copy_own(spot(0, 0)[2])
        else:
            for i in range(per_peer):
                x, _, slot = spot(0, i)
                pl.when(x == me_x)(functools.partial(copy_own, slot))

    def settle(ref, sem, count):
        if simple:
            block = ref.at[pl.ds(0, count)]
            pltpu.make_async_copy(block, block, sem).wait()
        else:
            block = ref.at[pl.ds(0, count - own)]
            pltpu.make_async_copy(block, block, sem).wait()

    total = boxes - 1 if simple else boxes

    def send_chunk(c):
        for j, i in blocks:
            remote(j, i, lambda: in_copy(c, j, i).start())

        def copy_own(slot):
            got[c, mine] = sent[c, slot]

        keep(copy_own)

    loads[1].wait()
    pieces.wait()
    project(0)

    pl.semaphore_wait(barrier, expected)
    for j, i in blocks:
        remote(j, i, lambda: phase_copy(j, i).start())

    def own_phase(slot):
        phase_in[pl.ds(pl.multiple_of(mine * 8, 8), 8), :] = phase_out[
            pl.ds(pl.multiple_of(slot * 8, 8), 8), :
        ]

    keep(own_phase)
    send_chunk(0)
    for j in range(1, count_y):
        last_copy(j).start()
    here = pl.ds(pl.multiple_of(me_y * 8, 8), 8)
    last_in[here, :] = last_out[here, :]
    send_chunk(1)

    @pl.loop(1, pairs)
    def _(cc):
        project(cc)
        send_chunk(cc * 2)
        send_chunk(cc * 2 + 1)

    loads[2].wait()
    loads[3].wait()
    settle_rows = 8 * total if simple else 8 * (total - own)
    rows_seen = phase_in.at[pl.ds(0, settle_rows), :]
    pltpu.make_async_copy(rows_seen, rows_seen, ang_recv.at[0]).wait()
    cosine, sine = cos_sin(phase_in[...])
    cs[...] = cosine
    sn[...] = sine
    rows_seen = last_in.at[pl.ds(0, 8 * (count_y - 1)), :]
    pltpu.make_async_copy(rows_seen, rows_seen, ang_recv.at[1]).wait()
    cosine, sine = cos_sin(last_in[...])
    cs_last[...] = cosine
    sn_last[...] = sine

    def wide(ref, row):
        return jnp.concatenate([ref[row : row + 1, :], ref[row + 1 : row + 2, :]], axis=1)

    def level(load, store, number, stride, phase):
        lows = [b for b in range(nx * ny) if b // stride % 2 == 0]
        low = jnp.concatenate([load(b) for b in lows], axis=0)
        high = jnp.concatenate([load(b + stride) for b in lows], axis=0)
        for h in range(2):
            prod = jnp.dot(low, w[number, h, :coeffs, :], preferred_element_type=f32)
            prod += jnp.dot(high, w[number, h, coeffs:, :], preferred_element_type=f32)
            values = []
            for index, b in enumerate(lows):
                base = index * 2 * SIDES
                upper, lower = prod[base : base + SIDES], prod[base + SIDES : base + 2 * SIDES]
                real = upper[:, :coeffs] - lower[:, coeffs:]
                imag = lower[:, :coeffs] + upper[:, coeffs:]
                values.append((b + h * stride, turn(real, imag, *phase(b + h * stride))))
            store(values)

    def into(ref):
        def store(values):
            for b, value in values:
                ref[b] = value

        return store

    def phases(number):
        return lambda b: (wide(cs, b * 8 + number * 2), wide(sn, b * 8 + number * 2))

    def last_phases(b):
        g, yy = b // ny, b % ny
        row = (yy * yl + g % yl) * 8 + g // yl * 2
        return wide(cs_last, row), wide(sn_last, row)

    def middle(c):
        settle(got.at[c], in_recv.at[c], total)
        level(lambda b: got[c, b], into(ping), 0, 4, phases(0))
        level(lambda b: ping[b], into(pong), 1, 2 * ny, phases(1))
        level(lambda b: pong[b], into(ping), 2, 2, phases(2))

        def store(values):
            for b, value in values:
                back[c, b // ny, b % ny] = value

        level(lambda b: ping[b], store, 3, ny, phases(3))
        for k in range(1, nx):
            out_copy(c, k).start()
        home[c, group] = back[c, group]

    def final(c):
        seen = home.at[c, pl.ds(0, nx - 1)]
        pltpu.make_async_copy(seen, seen, out_recv.at[c]).wait()
        first = pl.multiple_of(c * SIDES, SIDES)

        def store(values):
            rows = jnp.concatenate([value for _, value in values], axis=0)
            prod = jnp.dot(rows, interp[...], preferred_element_type=f32)
            for index, (b, _) in enumerate(values):
                g, yy = b // ny, b % ny
                base = index * 2 * SIDES
                upper, lower = prod[base : base + SIDES], prod[base + SIDES : base + 2 * SIDES]
                real = upper[:, :points] - lower[:, points:]
                imag = upper[:, points:] + lower[:, :points]
                slot = (yy * yl + g % yl) * per_peer + g // yl
                out_ref[slot, pl.ds(first, SIDES), :] = real.astype(bf16)
                out_ref[slot, pl.ds(first + sides, SIDES), :] = imag.astype(bf16)

        level(lambda b: home[c, b // ny, b % ny], store, 4, 1, last_phases)

    middle(0)

    @pl.loop(1, chunks)
    def _(c):
        middle(c)
        final(c - 1)

    final(chunks - 1)

    for c in range(chunks):
        settle(sent.at[c], in_send.at[c], total)
        seen = back.at[c, pl.ds(0, nx - 1)]
        pltpu.make_async_copy(seen, seen, out_send.at[c]).wait()
    rows_seen = phase_out.at[pl.ds(0, settle_rows), :]
    pltpu.make_async_copy(rows_seen, rows_seen, ang_send.at[0]).wait()
    rows_seen = last_out.at[pl.ds(0, 8 * (count_y - 1)), :]
    pltpu.make_async_copy(rows_seen, rows_seen, ang_send.at[1]).wait()


def local(sources, projection, translations, angles, interpolation, box_order):
    boxes, sides, points = sources.shape
    coeffs = projection.shape[1] // 2
    count_x, count_y = lax.axis_size("gx"), lax.axis_size("gy")
    chunks = sides // SIDES
    f32, bf16 = jnp.float32, jnp.bfloat16
    anywhere = pl.BlockSpec(memory_space=pltpu.HBM)
    vmem = pl.BlockSpec(memory_space=pltpu.VMEM)
    state = pltpu.VMEM((chunks, boxes, 2 * SIDES, coeffs), bf16)
    one = pltpu.VMEM((boxes, 2 * SIDES, coeffs), bf16)
    grouped = pltpu.VMEM((chunks, 4, boxes // 4, 2 * SIDES, coeffs), bf16)
    phases = pltpu.VMEM((boxes * 8, coeffs // 2), f32)
    last = pltpu.VMEM((count_y * 8, coeffs // 2), f32)
    dma = pltpu.SemaphoreType.DMA
    return pl.pallas_call(
        functools.partial(kernel, count_x, count_y, sides),
        out_shape=jax.ShapeDtypeStruct((boxes, 2 * sides, points), bf16),
        in_specs=[vmem] + [anywhere] * 5,
        out_specs=vmem,
        scratch_shapes=[
            pltpu.VMEM(angles.shape, f32), pltpu.VMEM(sources.shape, bf16),
            pltpu.VMEM(projection.shape, bf16), pltpu.VMEM(translations.shape, bf16),
            pltpu.VMEM(interpolation.shape, bf16), pltpu.SMEM((boxes,), jnp.int32),
            pltpu.VMEM((boxes, coeffs), f32), pltpu.VMEM((boxes, coeffs), f32),
            state, state, one, one, grouped, grouped,
            phases, phases, last, last, phases, phases, last, last,
            dma((5,)), dma((chunks,)), dma((chunks,)), dma((chunks,)),
            dma((chunks,)), dma((2,)), dma((2,)),
        ],
        compiler_params=pltpu.CompilerParams(
            collective_id=0, has_side_effects=True, vmem_limit_bytes=60 * 2**20
        ),
    )(
        box_order.reshape(1, boxes), angles, sources, projection, translations, interpolation
    )


def solution(mesh):
    placed = (
        P(("gx", "gy"), None, None),
        P(),
        P(),
        P(None, ("gx", "gy"), None),
        P(),
        P(("gx", "gy")),
    )
    return jax.shard_map(
        local, mesh=mesh, in_specs=placed, out_specs=P(("gx", "gy"), None, None), check_vma=False
    )
```

```python
import functools

import jax
import jax.numpy as jnp
from jax import lax
from jax.experimental import pallas as pl
from jax.experimental.pallas import tpu as pltpu
from jax.sharding import PartitionSpec as P

SIDES = 8
AHEAD = 2
STEP = 3.140625 / 32766
SIN = (1.0, -0.16666666666602138, 0.00833333096559207, -0.00019840860009446372,
       2.752520673490089e-06, -2.3888051249402636e-08)
COS = (1.0, -0.4999999999699515, 0.04166666647185967, -0.001388888415088631,
       2.480103815897482e-05, -2.752459905052806e-07, 1.9906439107985886e-09)


def level_plan(count_x, count_y):
    bits_x = count_x.bit_length() - 1
    bits_y = count_y.bit_length() - 1
    return [
        ("gy", bits_y - 1),
        ("gx", bits_x - 1),
        ("gy", bits_y - 2),
        ("gx", bits_x - 2),
        ("gy", bits_y - 3),
    ]


def cos_sin(angle):
    half = angle * 0.5
    square = half * half

    def poly(coefs):
        total = jnp.full_like(square, coefs[-1])
        for coef in coefs[-2::-1]:
            total = total * square + coef
        return total

    sine, cosine = half * poly(SIN), poly(COS)
    return 1.0 - 2.0 * (sine * sine), 2.0 * (sine * cosine)


def code(angle):
    return jnp.round(angle * (1 / STEP)).astype(jnp.int32).astype(jnp.int16)


def decode(value):
    return value.astype(jnp.int32).astype(jnp.float32) * STEP


def kernel(
    count_x, count_y, sides,
    order_ref, angles_hbm, src_hbm, proj_hbm, w_hbm, interp_hbm,
    out_ref,
    ang, src, proj, w, interp, inverse, c0, s0, sent, got, ping, pong, back, home,
    staged, staged_last, phase_out, phase_in, last_out, last_in, cs, sn, cs_last, sn_last,
    load_sem, in_send, in_recv, out_send, out_recv, ang_send, ang_recv,
):
    f32, bf16 = jnp.float32, jnp.bfloat16
    nx, ny = 4, 8
    boxes = src.shape[0]
    coeffs = proj.shape[1] // 2
    points = interp.shape[1] // 2
    per_peer = boxes // count_y
    xl, yl = count_x // nx, count_y // ny
    simple = xl == 1 and yl == 1
    chunks = sides // SIDES
    lanes = ang.shape[2] // 2
    me_x, me_y = lax.axis_index("gx"), lax.axis_index("gy")
    group, group_low = me_x // xl, me_x % xl
    mine = group * ny + me_y // yl

    def spot(j, i):
        p = (me_y + j) % count_y
        r = (me_x + i) % per_peer
        return group_low + xl * (r * yl + me_y % yl), p, p * per_peer + r

    def origin(k, m):
        x = group_low + xl * ((group + k) % nx)
        return x, group % yl + yl * ((me_y // yl + m) % ny)

    def onto(k):
        return (group + k) % nx

    def remote(j, i, act):
        if j or i % per_peer:
            if simple or j:
                act()
                return
        elif simple:
            return
        pl.when(spot(j, i)[0] != me_x)(act)

    barrier = pltpu.get_barrier_semaphore()
    expected = 0
    for k in range(nx):
        for m in range(ny):
            if simple and not (k or m):
                continue
            x, y = origin(k, m)
            if simple:
                pl.semaphore_signal(
                    barrier, inc=1, device_id=(x, y), device_id_type=pl.DeviceIdType.MESH
                )
            else:
                @pl.when((x != me_x) | (y != me_y))
                def _(x=x, y=y):
                    pl.semaphore_signal(
                        barrier, inc=1, device_id=(x, y), device_id_type=pl.DeviceIdType.MESH
                    )
    if simple:
        expected = nx * ny - 1
    else:
        for k in range(1, nx):
            pl.semaphore_signal(
                barrier, inc=1, device_id=(group_low + xl * onto(k), me_y),
                device_id_type=pl.DeviceIdType.MESH,
            )
        for m in range(1, count_y):
            pl.semaphore_signal(
                barrier, inc=1, device_id=(me_x, (me_y + m) % count_y),
                device_id_type=pl.DeviceIdType.MESH,
            )
        own = (me_x // xl % yl == me_y % yl).astype(jnp.int32)
        expected = nx * ny - own + nx - 1 + count_y - 1

    pairs = chunks // 2
    loads = [
        pltpu.make_async_copy(angles_hbm, ang, load_sem.at[0]),
        pltpu.make_async_copy(proj_hbm, proj, load_sem.at[1]),
        pltpu.make_async_copy(interp_hbm, interp, load_sem.at[2]),
        pltpu.make_async_copy(w_hbm, w, load_sem.at[3]),
    ]
    pieces = pltpu.make_async_copy(src_hbm, src, load_sem.at[4])
    loads[0].start()
    loads[1].start()
    pieces.start()
    loads[3].start()
    loads[2].start()

    local = order_ref[...] % boxes
    place = lax.broadcasted_iota(jnp.int32, local.shape, 1)
    for slot in range(boxes):
        inverse[slot] = jnp.max(jnp.where(local == slot, place, 0))

    loads[0].wait()
    for first in range(0, boxes, 8):
        for level in range(4):
            for part in range(2):
                staged[pl.ds(first * 8 + level * 2 + part, 8, stride=8), :] = ang[
                    level + 1, first : first + 8, part * lanes : (part + 1) * lanes
                ]
    for slot in range(boxes):
        for part in range(2):
            row = slot // per_peer * 8 + slot % per_peer * 2 + part
            staged_last[row : row + 1, :] = ang[
                5, slot : slot + 1, part * lanes : (part + 1) * lanes
            ]
    for slot in range(boxes):
        phase_out[slot] = code(staged[slot * 8 : slot * 8 + 8, :])
    for p in range(count_y):
        last_out[p] = code(staged_last[p * 8 : p * 8 + 8, :])
    cosine, sine = cos_sin(ang[0])
    c0[...] = cosine
    s0[...] = sine

    def turn(real, imag, cosine, sine):
        return jnp.concatenate(
            [cosine * real - sine * imag, sine * real + cosine * imag], axis=0
        ).astype(bf16)

    def project(cc):
        first = pl.multiple_of(cc * 2 * SIDES, 2 * SIDES)
        for half in range(2):
            slots = range(half * boxes // 2, (half + 1) * boxes // 2)
            rows = jnp.concatenate(
                [src[inverse[slot], pl.ds(first, 2 * SIDES), :] for slot in slots], axis=0
            )
            prod = jnp.dot(rows, proj[...], preferred_element_type=f32)
            for index, slot in enumerate(slots):
                for part in range(2):
                    at = (index * 2 + part) * SIDES
                    block = prod[at : at + SIDES]
                    sent[cc * 2 + part, slot] = turn(
                        block[:, :coeffs], block[:, coeffs:],
                        c0[slot : slot + 1, :], s0[slot : slot + 1, :],
                    )

    def in_copy(c, j, i):
        x, y, slot = spot(j, i)
        return pltpu.make_async_remote_copy(
            src_ref=sent.at[c, slot], dst_ref=got.at[c, mine],
            send_sem=in_send.at[c], recv_sem=in_recv.at[c],
            device_id=(x, y), device_id_type=pl.DeviceIdType.MESH,
        )

    def phase_copy(j, i):
        x, y, slot = spot(j, i)
        return pltpu.make_async_remote_copy(
            src_ref=phase_out.at[slot], dst_ref=phase_in.at[mine],
            send_sem=ang_send.at[0], recv_sem=ang_recv.at[0],
            device_id=(x, y), device_id_type=pl.DeviceIdType.MESH,
        )

    def last_copy(j):
        p = (me_y + j) % count_y
        return pltpu.make_async_remote_copy(
            src_ref=last_out.at[p], dst_ref=last_in.at[me_y],
            send_sem=ang_send.at[1], recv_sem=ang_recv.at[1],
            device_id=(me_x, p), device_id_type=pl.DeviceIdType.MESH,
        )

    def out_copy(c, k):
        return pltpu.make_async_remote_copy(
            src_ref=back.at[c, onto(k)], dst_ref=home.at[c, group],
            send_sem=out_send.at[c], recv_sem=out_recv.at[c],
            device_id=(group_low + xl * onto(k), me_y), device_id_type=pl.DeviceIdType.MESH,
        )

    far = sorted(range(count_y), key=lambda j: -min(j, count_y - j))
    blocks = [(j, i) for j in far for i in range(per_peer)]

    def keep(copy_own):
        if simple:
            copy_own(spot(0, 0)[2])
        else:
            for i in range(per_peer):
                x, _, slot = spot(0, i)
                pl.when(x == me_x)(functools.partial(copy_own, slot))

    def settle(ref, sem, count):
        if simple:
            block = ref.at[pl.ds(0, count)]
            pltpu.make_async_copy(block, block, sem).wait()
        else:
            block = ref.at[pl.ds(0, count - own)]
            pltpu.make_async_copy(block, block, sem).wait()

    total = boxes - 1 if simple else boxes

    def send_chunk(c):
        for j, i in blocks:
            remote(j, i, lambda: in_copy(c, j, i).start())

        def copy_own(slot):
            got[c, mine] = sent[c, slot]

        keep(copy_own)

    loads[1].wait()
    pieces.wait()
    project(0)

    pl.semaphore_wait(barrier, expected)
    for j, i in blocks:
        remote(j, i, lambda: phase_copy(j, i).start())

    def own_phase(slot):
        phase_in[mine] = phase_out[slot]

    keep(own_phase)
    send_chunk(0)
    for j in range(1, count_y):
        last_copy(j).start()
    last_in[me_y] = last_out[me_y]
    send_chunk(1)

    @pl.loop(1, pairs)
    def _(cc):
        project(cc)

    loads[2].wait()
    loads[3].wait()
    settle(phase_in, ang_recv.at[0], total)
    cosine, sine = cos_sin(decode(phase_in[...]))
    cs[...] = cosine
    sn[...] = sine
    seen = last_in.at[pl.ds(0, count_y - 1)]
    pltpu.make_async_copy(seen, seen, ang_recv.at[1]).wait()
    cosine, sine = cos_sin(decode(last_in[...]))
    cs_last[...] = cosine
    sn_last[...] = sine

    def wide(ref, block, row):
        return jnp.concatenate(
            [ref[block, row : row + 1, :], ref[block, row + 1 : row + 2, :]], axis=1
        )

    def level(load, store, number, stride, phase):
        lows = [b for b in range(nx * ny) if b // stride % 2 == 0]
        low = jnp.concatenate([load(b) for b in lows], axis=0)
        high = jnp.concatenate([load(b + stride) for b in lows], axis=0)
        for h in range(2):
            prod = jnp.dot(low, w[number, h, :coeffs, :], preferred_element_type=f32)
            prod += jnp.dot(high, w[number, h, coeffs:, :], preferred_element_type=f32)
            values = []
            for index, b in enumerate(lows):
                base = index * 2 * SIDES
                upper, lower = prod[base : base + SIDES], prod[base + SIDES : base + 2 * SIDES]
                real = upper[:, :coeffs] - lower[:, coeffs:]
                imag = lower[:, :coeffs] + upper[:, coeffs:]
                values.append((b + h * stride, turn(real, imag, *phase(b + h * stride))))
            store(values)

    def into(ref):
        def store(values):
            for b, value in values:
                ref[b] = value

        return store

    def phases(number):
        return lambda b: (wide(cs, b, number * 2), wide(sn, b, number * 2))

    def last_phases(b):
        g, yy = b // ny, b % ny
        y, row = yy * yl + g % yl, g // yl * 2
        return wide(cs_last, y, row), wide(sn_last, y, row)

    def middle(c):
        settle(got.at[c], in_recv.at[c], total)

        @pl.when(c + AHEAD < chunks)
        def _():
            send_chunk(c + AHEAD)

        level(lambda b: got[c, b], into(ping), 0, 4, phases(0))
        level(lambda b: ping[b], into(pong), 1, 2 * ny, phases(1))
        level(lambda b: pong[b], into(ping), 2, 2, phases(2))

        def store(values):
            for b, value in values:
                back[c, b // ny, b % ny] = value

        level(lambda b: ping[b], store, 3, ny, phases(3))
        for k in range(1, nx):
            out_copy(c, k).start()
        home[c, group] = back[c, group]

    def final(c):
        seen = home.at[c, pl.ds(0, nx - 1)]
        pltpu.make_async_copy(seen, seen, out_recv.at[c]).wait()
        first = pl.multiple_of(c * SIDES, SIDES)

        def store(values):
            rows = jnp.concatenate([value for _, value in values], axis=0)
            prod = jnp.dot(rows, interp[...], preferred_element_type=f32)
            for index, (b, _) in enumerate(values):
                g, yy = b // ny, b % ny
                base = index * 2 * SIDES
                upper, lower = prod[base : base + SIDES], prod[base + SIDES : base + 2 * SIDES]
                real = upper[:, :points] - lower[:, points:]
                imag = upper[:, points:] + lower[:, :points]
                slot = (yy * yl + g % yl) * per_peer + g // yl
                out_ref[slot, pl.ds(first, SIDES), :] = real.astype(bf16)
                out_ref[slot, pl.ds(first + sides, SIDES), :] = imag.astype(bf16)

        level(lambda b: home[c, b // ny, b % ny], store, 4, 1, last_phases)

    middle(0)

    @pl.loop(1, chunks)
    def _(c):
        middle(c)
        final(c - 1)

    final(chunks - 1)

    for c in range(chunks):
        settle(sent.at[c], in_send.at[c], total)
        seen = back.at[c, pl.ds(0, nx - 1)]
        pltpu.make_async_copy(seen, seen, out_send.at[c]).wait()
    settle(phase_out, ang_send.at[0], total)
    seen = last_out.at[pl.ds(0, count_y - 1)]
    pltpu.make_async_copy(seen, seen, ang_send.at[1]).wait()


def local(sources, projection, translations, angles, interpolation, box_order):
    boxes, sides, points = sources.shape
    coeffs = projection.shape[1] // 2
    count_x, count_y = lax.axis_size("gx"), lax.axis_size("gy")
    chunks = sides // SIDES
    f32, bf16 = jnp.float32, jnp.bfloat16
    anywhere = pl.BlockSpec(memory_space=pltpu.HBM)
    vmem = pl.BlockSpec(memory_space=pltpu.VMEM)
    state = pltpu.VMEM((chunks, boxes, 2 * SIDES, coeffs), bf16)
    one = pltpu.VMEM((boxes, 2 * SIDES, coeffs), bf16)
    grouped = pltpu.VMEM((chunks, 4, boxes // 4, 2 * SIDES, coeffs), bf16)
    lanes = coeffs // 2
    phases, last = pltpu.VMEM((boxes, 8, lanes), f32), pltpu.VMEM((count_y, 8, lanes), f32)
    coded, coded_last = (
        pltpu.VMEM((boxes, 8, lanes), jnp.int16), pltpu.VMEM((count_y, 8, lanes), jnp.int16)
    )
    dma = pltpu.SemaphoreType.DMA
    return pl.pallas_call(
        functools.partial(kernel, count_x, count_y, sides),
        out_shape=pltpu.VMEM((boxes, 2 * sides, points), bf16),
        in_specs=[vmem] + [anywhere] * 5,
        out_specs=vmem,
        scratch_shapes=[
            pltpu.VMEM(angles.shape, f32), pltpu.VMEM(sources.shape, bf16),
            pltpu.VMEM(projection.shape, bf16), pltpu.VMEM(translations.shape, bf16),
            pltpu.VMEM(interpolation.shape, bf16), pltpu.SMEM((boxes,), jnp.int32),
            pltpu.VMEM((boxes, coeffs), f32), pltpu.VMEM((boxes, coeffs), f32),
            state, state, one, one, grouped, grouped,
            pltpu.VMEM((boxes * 8, lanes), f32), pltpu.VMEM((count_y * 8, lanes), f32),
            coded, coded, coded_last, coded_last, phases, phases, last, last,
            dma((5,)), dma((chunks,)), dma((chunks,)), dma((chunks,)),
            dma((chunks,)), dma((2,)), dma((2,)),
        ],
        compiler_params=pltpu.CompilerParams(
            collective_id=0, has_side_effects=True, vmem_limit_bytes=40 * 2**20
        ),
    )(
        *[
            pltpu.with_memory_space_constraint(value, pltpu.HBM)
            for value in (
                box_order.reshape(1, boxes), angles, sources, projection, translations,
                interpolation,
            )
        ]
    )


def solution(mesh):
    placed = (
        P(("gx", "gy"), None, None),
        P(),
        P(),
        P(None, ("gx", "gy"), None),
        P(),
        P(("gx", "gy")),
    )
    return jax.shard_map(
        local, mesh=mesh, in_specs=placed, out_specs=P(("gx", "gy"), None, None), check_vma=False
    )
```

```python
import functools

import jax
import jax.numpy as jnp
from jax import lax
from jax.experimental import pallas as pl
from jax.experimental.pallas import tpu as pltpu
from jax.sharding import PartitionSpec as P

SIDES = 8
AHEAD = 2
STEP = 3.140625 / 32766
SIN = (1.0, -0.16666666666602138, 0.00833333096559207, -0.00019840860009446372,
       2.752520673490089e-06, -2.3888051249402636e-08)
COS = (1.0, -0.4999999999699515, 0.04166666647185967, -0.001388888415088631,
       2.480103815897482e-05, -2.752459905052806e-07, 1.9906439107985886e-09)


def level_plan(count_x, count_y):
    bits_x = count_x.bit_length() - 1
    bits_y = count_y.bit_length() - 1
    return [
        ("gy", bits_y - 1),
        ("gx", bits_x - 1),
        ("gy", bits_y - 2),
        ("gx", bits_x - 2),
        ("gy", bits_y - 3),
    ]


def cos_sin(angle):
    half = angle * 0.5
    square = half * half

    def poly(coefs):
        total = jnp.full_like(square, coefs[-1])
        for coef in coefs[-2::-1]:
            total = total * square + coef
        return total

    sine, cosine = half * poly(SIN), poly(COS)
    return 1.0 - 2.0 * (sine * sine), 2.0 * (sine * cosine)


def code(angle):
    return jnp.round(angle * (1 / STEP)).astype(jnp.int32).astype(jnp.int16)


def decode(value):
    return value.astype(jnp.int32).astype(jnp.float32) * STEP


def kernel(
    count_x, count_y, sides,
    order_ref, angles_hbm, src_hbm, proj_hbm, w_hbm, interp_hbm,
    out_ref,
    ang, src, proj, w, interp, inverse, c0, s0, sent, got, ping, pong, back, home,
    staged, staged_last, phase_out, phase_in, last_out, last_in, cs, sn, cs_last, sn_last,
    ready, load_sem, in_send, in_recv, out_send, out_recv, ang_send, ang_recv,
):
    f32, bf16 = jnp.float32, jnp.bfloat16
    nx, ny = 4, 8
    boxes = src.shape[0]
    coeffs = proj.shape[1] // 2
    points = interp.shape[1] // 2
    per_peer = boxes // count_y
    xl, yl = count_x // nx, count_y // ny
    simple = xl == 1 and yl == 1
    chunks = sides // SIDES
    lanes = ang.shape[2] // 2
    me_x, me_y = lax.axis_index("gx"), lax.axis_index("gy")
    group, group_low = me_x // xl, me_x % xl
    mine = group * ny + me_y // yl

    def spot(j, i):
        p = (me_y + j) % count_y
        r = (me_x + i) % per_peer
        return group_low + xl * (r * yl + me_y % yl), p, p * per_peer + r

    def origin(k, m):
        x = group_low + xl * ((group + k) % nx)
        return x, group % yl + yl * ((me_y // yl + m) % ny)

    def onto(k):
        return (group + k) % nx

    def remote(j, i, act):
        if j or i % per_peer:
            if simple or j:
                act()
                return
        elif simple:
            return
        pl.when(spot(j, i)[0] != me_x)(act)

    barrier = pltpu.get_barrier_semaphore()
    expected = 0
    for k in range(nx):
        for m in range(ny):
            if simple and (k == 0) == (m == 0):
                continue
            x, y = origin(k, m)
            if simple:
                pl.semaphore_signal(
                    barrier, inc=1, device_id=(x, y), device_id_type=pl.DeviceIdType.MESH
                )
            else:
                @pl.when((x != me_x) | (y != me_y))
                def _(x=x, y=y):
                    pl.semaphore_signal(
                        barrier, inc=1, device_id=(x, y), device_id_type=pl.DeviceIdType.MESH
                    )
    if simple:
        expected = nx - 1 + ny - 1
    else:
        for k in range(1, nx):
            pl.semaphore_signal(
                barrier, inc=1, device_id=(group_low + xl * onto(k), me_y),
                device_id_type=pl.DeviceIdType.MESH,
            )
        for m in range(1, count_y):
            pl.semaphore_signal(
                barrier, inc=1, device_id=(me_x, (me_y + m) % count_y),
                device_id_type=pl.DeviceIdType.MESH,
            )
        own = (me_x // xl % yl == me_y % yl).astype(jnp.int32)
        expected = nx * ny - own + nx - 1 + count_y - 1

    pairs = chunks // 2
    loads = [
        pltpu.make_async_copy(angles_hbm, ang, load_sem.at[0]),
        pltpu.make_async_copy(proj_hbm, proj, load_sem.at[1]),
        pltpu.make_async_copy(interp_hbm, interp, load_sem.at[2]),
        pltpu.make_async_copy(w_hbm, w, load_sem.at[3]),
    ]
    pieces = pltpu.make_async_copy(src_hbm, src, load_sem.at[4])
    loads[0].start()
    loads[1].start()
    pieces.start()
    loads[3].start()
    loads[2].start()

    local = order_ref[...] % boxes
    place = lax.broadcasted_iota(jnp.int32, local.shape, 1)
    for slot in range(boxes):
        inverse[slot] = jnp.max(jnp.where(local == slot, place, 0))

    loads[0].wait()
    for first in range(0, boxes, 8):
        for level in range(4):
            for part in range(2):
                staged[pl.ds(first * 8 + level * 2 + part, 8, stride=8), :] = ang[
                    level + 1, first : first + 8, part * lanes : (part + 1) * lanes
                ]
    for slot in range(boxes):
        for part in range(2):
            row = slot // per_peer * 8 + slot % per_peer * 2 + part
            staged_last[row : row + 1, :] = ang[
                5, slot : slot + 1, part * lanes : (part + 1) * lanes
            ]
    for slot in range(boxes):
        phase_out[slot] = code(staged[slot * 8 : slot * 8 + 8, :])
    for p in range(count_y):
        last_out[p] = code(staged_last[p * 8 : p * 8 + 8, :])
    cosine, sine = cos_sin(ang[0])
    c0[...] = cosine
    s0[...] = sine

    def turn(real, imag, cosine, sine):
        return jnp.concatenate(
            [cosine * real - sine * imag, sine * real + cosine * imag], axis=0
        ).astype(bf16)

    def project(cc):
        first = pl.multiple_of(cc * 2 * SIDES, 2 * SIDES)
        for half in range(2):
            slots = range(half * boxes // 2, (half + 1) * boxes // 2)
            rows = jnp.concatenate(
                [src[inverse[slot], pl.ds(first, 2 * SIDES), :] for slot in slots], axis=0
            )
            prod = jnp.dot(rows, proj[...], preferred_element_type=f32)
            for index, slot in enumerate(slots):
                for part in range(2):
                    at = (index * 2 + part) * SIDES
                    block = prod[at : at + SIDES]
                    sent[cc * 2 + part, slot] = turn(
                        block[:, :coeffs], block[:, coeffs:],
                        c0[slot : slot + 1, :], s0[slot : slot + 1, :],
                    )

    def in_copy(c, j, i):
        x, y, slot = spot(j, i)
        return pltpu.make_async_remote_copy(
            src_ref=sent.at[c, slot], dst_ref=got.at[c, mine],
            send_sem=in_send.at[c], recv_sem=in_recv.at[c],
            device_id=(x, y), device_id_type=pl.DeviceIdType.MESH,
        )

    def phase_copy(j, i):
        x, y, slot = spot(j, i)
        return pltpu.make_async_remote_copy(
            src_ref=phase_out.at[slot], dst_ref=phase_in.at[mine],
            send_sem=ang_send.at[0], recv_sem=ang_recv.at[0],
            device_id=(x, y), device_id_type=pl.DeviceIdType.MESH,
        )

    def last_copy(j):
        p = (me_y + j) % count_y
        return pltpu.make_async_remote_copy(
            src_ref=last_out.at[p], dst_ref=last_in.at[me_y],
            send_sem=ang_send.at[1], recv_sem=ang_recv.at[1],
            device_id=(me_x, p), device_id_type=pl.DeviceIdType.MESH,
        )

    def out_copy(c, odd, k):
        return pltpu.make_async_remote_copy(
            src_ref=back.at[c, odd, onto(k)], dst_ref=home.at[c, odd, group],
            send_sem=out_send.at[c, odd], recv_sem=out_recv.at[c, odd],
            device_id=(group_low + xl * onto(k), me_y), device_id_type=pl.DeviceIdType.MESH,
        )

    far = sorted(range(count_y), key=lambda j: -min(j, count_y - j))
    blocks = [(j, i) for j in far for i in range(per_peer)]

    def keep(copy_own):
        if simple:
            copy_own(spot(0, 0)[2])
        else:
            for i in range(per_peer):
                x, _, slot = spot(0, i)
                pl.when(x == me_x)(functools.partial(copy_own, slot))

    def settle(ref, sem, count):
        if simple:
            block = ref.at[pl.ds(0, count)]
            pltpu.make_async_copy(block, block, sem).wait()
        else:
            block = ref.at[pl.ds(0, count - own)]
            pltpu.make_async_copy(block, block, sem).wait()

    total = boxes - 1 if simple else boxes

    def send_part(c, part):
        for j, i in part:
            remote(j, i, lambda: in_copy(c, j, i).start())

    def keep_chunk(c):
        def copy_own(slot):
            got[c, mine] = sent[c, slot]

        keep(copy_own)

    def send_chunk(c):
        send_part(c, blocks)
        keep_chunk(c)

    loads[1].wait()
    pieces.wait()
    project(0)

    near = [(j, i) for j, i in blocks if j == 0 or i == 0] if simple else blocks
    others = [(j, i) for j, i in blocks if j and i] if simple else []
    pl.semaphore_wait(barrier, expected)
    if simple:
        for k in range(1, nx):
            pl.semaphore_signal(
                ready, inc=1, device_id=(onto(k), me_y), device_id_type=pl.DeviceIdType.MESH
            )
    for j, i in near:
        remote(j, i, lambda: phase_copy(j, i).start())
    send_part(0, near)
    for j in range(1, count_y):
        last_copy(j).start()
    send_part(1, near)

    def own_phase(slot):
        phase_in[mine] = phase_out[slot]

    keep(own_phase)
    last_in[me_y] = last_out[me_y]
    keep_chunk(0)
    keep_chunk(1)
    if simple:
        pl.semaphore_wait(ready, nx - 1)
    for j, i in others:
        remote(j, i, lambda: phase_copy(j, i).start())
    send_part(0, others)
    send_part(1, others)

    @pl.loop(1, pairs)
    def _(cc):
        project(cc)

    loads[2].wait()
    loads[3].wait()
    settle(phase_in, ang_recv.at[0], total)
    cosine, sine = cos_sin(decode(phase_in[...]))
    cs[...] = cosine
    sn[...] = sine
    seen = last_in.at[pl.ds(0, count_y - 1)]
    pltpu.make_async_copy(seen, seen, ang_recv.at[1]).wait()
    cosine, sine = cos_sin(decode(last_in[...]))
    cs_last[...] = cosine
    sn_last[...] = sine

    def wide(ref, block, row):
        return jnp.concatenate(
            [ref[block, row : row + 1, :], ref[block, row + 1 : row + 2, :]], axis=1
        )

    def level(load, store, number, stride, phase, odd=(0, 1)):
        lows = [b for b in range(nx * ny) if b // stride % 2 == 0 and b % 2 in odd]
        low = jnp.concatenate([load(b) for b in lows], axis=0)
        high = jnp.concatenate([load(b + stride) for b in lows], axis=0)
        for h in range(2):
            prod = jnp.dot(low, w[number, h, :coeffs, :], preferred_element_type=f32)
            prod += jnp.dot(high, w[number, h, coeffs:, :], preferred_element_type=f32)
            values = []
            for index, b in enumerate(lows):
                base = index * 2 * SIDES
                upper, lower = prod[base : base + SIDES], prod[base + SIDES : base + 2 * SIDES]
                real = upper[:, :coeffs] - lower[:, coeffs:]
                imag = lower[:, :coeffs] + upper[:, coeffs:]
                values.append((b + h * stride, turn(real, imag, *phase(b + h * stride))))
            store(values)

    def into(ref):
        def store(values):
            for b, value in values:
                ref[b] = value

        return store

    def phases(number):
        return lambda b: (wide(cs, b, number * 2), wide(sn, b, number * 2))

    def last_phases(b):
        g, yy = b // ny, b % ny
        y, row = yy * yl + g % yl, g // yl * 2
        return wide(cs_last, y, row), wide(sn_last, y, row)

    def middle(c):
        settle(got.at[c], in_recv.at[c], total)

        @pl.when(c + AHEAD < chunks)
        def _():
            send_chunk(c + AHEAD)


        def store(values):
            for b, value in values:
                back[c, b % 2, b // ny, b % ny // 2] = value

        for odd in range(2):
            level(lambda b: got[c, b], into(ping), 0, 4, phases(0), (odd,))
            level(lambda b: ping[b], into(pong), 1, 2 * ny, phases(1), (odd,))
            level(lambda b: pong[b], into(ping), 2, 2, phases(2), (odd,))
            level(lambda b: ping[b], store, 3, ny, phases(3), (odd,))
            for k in range(1, nx):
                out_copy(c, odd, k).start()
            home[c, odd, group] = back[c, odd, group]

    def final(c):
        for odd in range(2):
            seen = home.at[c, odd, pl.ds(0, nx - 1)]
            pltpu.make_async_copy(seen, seen, out_recv.at[c, odd]).wait()
        first = pl.multiple_of(c * SIDES, SIDES)

        def store(values):
            rows = jnp.concatenate([value for _, value in values], axis=0)
            prod = jnp.dot(rows, interp[...], preferred_element_type=f32)
            for index, (b, _) in enumerate(values):
                g, yy = b // ny, b % ny
                base = index * 2 * SIDES
                upper, lower = prod[base : base + SIDES], prod[base + SIDES : base + 2 * SIDES]
                real = upper[:, :points] - lower[:, points:]
                imag = upper[:, points:] + lower[:, :points]
                slot = (yy * yl + g % yl) * per_peer + g // yl
                out_ref[slot, pl.ds(first, SIDES), :] = real.astype(bf16)
                out_ref[slot, pl.ds(first + sides, SIDES), :] = imag.astype(bf16)

        level(lambda b: home[c, b % 2, b // ny, b % ny // 2], store, 4, 1, last_phases)

    middle(0)

    @pl.loop(1, chunks)
    def _(c):
        middle(c)
        final(c - 1)

    for c in range(chunks):
        settle(sent.at[c], in_send.at[c], total)
        for odd in range(2):
            seen = back.at[c, odd, pl.ds(0, nx - 1)]
            pltpu.make_async_copy(seen, seen, out_send.at[c, odd]).wait()
    settle(phase_out, ang_send.at[0], total)
    seen = last_out.at[pl.ds(0, count_y - 1)]
    pltpu.make_async_copy(seen, seen, ang_send.at[1]).wait()

    final(chunks - 1)


def local(sources, projection, translations, angles, interpolation, box_order):
    boxes, sides, points = sources.shape
    coeffs = projection.shape[1] // 2
    count_x, count_y = lax.axis_size("gx"), lax.axis_size("gy")
    chunks = sides // SIDES
    f32, bf16 = jnp.float32, jnp.bfloat16
    anywhere = pl.BlockSpec(memory_space=pltpu.HBM)
    vmem = pl.BlockSpec(memory_space=pltpu.VMEM)
    state = pltpu.VMEM((chunks, boxes, 2 * SIDES, coeffs), bf16)
    one = pltpu.VMEM((boxes, 2 * SIDES, coeffs), bf16)
    grouped = pltpu.VMEM((chunks, 2, 4, boxes // 8, 2 * SIDES, coeffs), bf16)
    lanes = coeffs // 2
    phases, last = pltpu.VMEM((boxes, 8, lanes), f32), pltpu.VMEM((count_y, 8, lanes), f32)
    coded, coded_last = (
        pltpu.VMEM((boxes, 8, lanes), jnp.int16), pltpu.VMEM((count_y, 8, lanes), jnp.int16)
    )
    dma = pltpu.SemaphoreType.DMA
    return pl.pallas_call(
        functools.partial(kernel, count_x, count_y, sides),
        out_shape=pltpu.VMEM((boxes, 2 * sides, points), bf16),
        in_specs=[vmem] + [anywhere] * 5,
        out_specs=vmem,
        scratch_shapes=[
            pltpu.VMEM(angles.shape, f32), pltpu.VMEM(sources.shape, bf16),
            pltpu.VMEM(projection.shape, bf16), pltpu.VMEM(translations.shape, bf16),
            pltpu.VMEM(interpolation.shape, bf16), pltpu.SMEM((boxes,), jnp.int32),
            pltpu.VMEM((boxes, coeffs), f32), pltpu.VMEM((boxes, coeffs), f32),
            state, state, one, one, grouped, grouped,
            pltpu.VMEM((boxes * 8, lanes), f32), pltpu.VMEM((count_y * 8, lanes), f32),
            coded, coded, coded_last, coded_last, phases, phases, last, last,
            pltpu.SemaphoreType.REGULAR, dma((5,)), dma((chunks,)), dma((chunks,)), dma((chunks, 2)),
            dma((chunks, 2)), dma((2,)), dma((2,)),
        ],
        compiler_params=pltpu.CompilerParams(
            collective_id=0, has_side_effects=True, vmem_limit_bytes=40 * 2**20
        ),
    )(
        *[
            pltpu.with_memory_space_constraint(value, pltpu.HBM)
            for value in (
                box_order.reshape(1, boxes), angles, sources, projection, translations,
                interpolation,
            )
        ]
    )


def solution(mesh):
    placed = (
        P(("gx", "gy"), None, None),
        P(),
        P(),
        P(None, ("gx", "gy"), None),
        P(),
        P(("gx", "gy")),
    )
    return jax.shard_map(
        local, mesh=mesh, in_specs=placed, out_specs=P(("gx", "gy"), None, None), check_vma=False
    )
```

```python
import functools

import jax
import jax.numpy as jnp
from jax import lax
from jax.experimental import pallas as pl
from jax.experimental.pallas import tpu as pltpu
from jax.sharding import PartitionSpec as P

SIDES = 8
AHEAD = 2
STEP = 3.140625 / 32766
SIN = (1.0, -0.16666666666602138, 0.00833333096559207, -0.00019840860009446372,
       2.752520673490089e-06, -2.3888051249402636e-08)
COS = (1.0, -0.4999999999699515, 0.04166666647185967, -0.001388888415088631,
       2.480103815897482e-05, -2.752459905052806e-07, 1.9906439107985886e-09)


def level_plan(count_x, count_y):
    bits_x = count_x.bit_length() - 1
    bits_y = count_y.bit_length() - 1
    return [
        ("gy", bits_y - 1),
        ("gx", bits_x - 1),
        ("gy", bits_y - 2),
        ("gx", bits_x - 2),
        ("gy", bits_y - 3),
    ]


def cos_sin(angle):
    half = angle * 0.5
    square = half * half

    def poly(coefs):
        total = jnp.full_like(square, coefs[-1])
        for coef in coefs[-2::-1]:
            total = total * square + coef
        return total

    sine, cosine = half * poly(SIN), poly(COS)
    return 1.0 - 2.0 * (sine * sine), 2.0 * (sine * cosine)


def code(angle):
    return jnp.round(angle * (1 / STEP)).astype(jnp.int32).astype(jnp.int16)


def decode(value):
    return value.astype(jnp.int32).astype(jnp.float32) * STEP


def kernel(
    count_x, count_y, sides,
    order_ref, angles_hbm, src_hbm, proj_hbm, w_hbm, interp_hbm,
    out_ref,
    ang, src, proj, w, interp, inverse, c0, s0, sent, got, ping, pong, back, home,
    staged, staged_last, phase_out, phase_in, last_out, last_in, cs, sn, cs_last, sn_last,
    ready, load_sem, in_send, in_recv, out_send, out_recv, ang_send, ang_recv,
):
    f32, bf16 = jnp.float32, jnp.bfloat16
    nx, ny = 4, 8
    boxes = src.shape[0]
    coeffs = proj.shape[1] // 2
    points = interp.shape[1] // 2
    per_peer = boxes // count_y
    xl, yl = count_x // nx, count_y // ny
    simple = xl == 1 and yl == 1
    chunks = sides // SIDES
    lanes = ang.shape[2] // 2
    me_x, me_y = lax.axis_index("gx"), lax.axis_index("gy")
    group, group_low = me_x // xl, me_x % xl
    mine = group * ny + me_y // yl

    def spot(j, i):
        p = (me_y // 2 + j // 2) % (count_y // 2) * 2 + (me_y + j) % 2
        r = (me_x + i) % per_peer
        return group_low + xl * (r * yl + me_y % yl), p, p * per_peer + r

    def origin(k, m):
        x = group_low + xl * ((group + k) % nx)
        return x, group % yl + yl * ((me_y // yl + m) % ny)

    def onto(k):
        return (group + k) % nx

    def remote(j, i, act):
        if j or i % per_peer:
            if simple or j:
                act()
                return
        elif simple:
            return
        pl.when(spot(j, i)[0] != me_x)(act)

    barrier = pltpu.get_barrier_semaphore()
    expected = 0
    for k in range(nx):
        for m in range(ny):
            if simple and (k == 0) == (m == 0):
                continue
            x, y = origin(k, m)
            if simple:
                pl.semaphore_signal(
                    barrier, inc=1, device_id=(x, y), device_id_type=pl.DeviceIdType.MESH
                )
            else:
                @pl.when((x != me_x) | (y != me_y))
                def _(x=x, y=y):
                    pl.semaphore_signal(
                        barrier, inc=1, device_id=(x, y), device_id_type=pl.DeviceIdType.MESH
                    )
    if simple:
        expected = nx - 1 + ny - 1
    else:
        for k in range(1, nx):
            pl.semaphore_signal(
                barrier, inc=1, device_id=(group_low + xl * onto(k), me_y),
                device_id_type=pl.DeviceIdType.MESH,
            )
        for m in range(1, count_y):
            pl.semaphore_signal(
                barrier, inc=1, device_id=(me_x, (me_y + m) % count_y),
                device_id_type=pl.DeviceIdType.MESH,
            )
        own = (me_x // xl % yl == me_y % yl).astype(jnp.int32)
        expected = nx * ny - own + nx - 1 + count_y - 1

    pairs = chunks // 2
    loads = [
        pltpu.make_async_copy(angles_hbm, ang, load_sem.at[0]),
        pltpu.make_async_copy(proj_hbm, proj, load_sem.at[1]),
        pltpu.make_async_copy(interp_hbm, interp, load_sem.at[2]),
        pltpu.make_async_copy(w_hbm, w, load_sem.at[3]),
    ]
    pieces = pltpu.make_async_copy(src_hbm, src, load_sem.at[4])
    loads[0].start()
    loads[1].start()
    pieces.start()
    loads[3].start()
    loads[2].start()

    local = order_ref[...] % boxes
    place = lax.broadcasted_iota(jnp.int32, local.shape, 1)
    for slot in range(boxes):
        inverse[slot] = jnp.max(jnp.where(local == slot, place, 0))

    loads[0].wait()
    for first in range(0, boxes, 8):
        for level in range(4):
            for part in range(2):
                staged[pl.ds(first * 8 + level * 2 + part, 8, stride=8), :] = ang[
                    level + 1, first : first + 8, part * lanes : (part + 1) * lanes
                ]
    for slot in range(boxes):
        for part in range(2):
            row = slot // per_peer * 8 + slot % per_peer * 2 + part
            staged_last[row : row + 1, :] = ang[
                5, slot : slot + 1, part * lanes : (part + 1) * lanes
            ]
    for slot in range(boxes):
        phase_out[slot] = code(staged[slot * 8 : slot * 8 + 8, :])
    for p in range(count_y):
        last_out[p] = code(staged_last[p * 8 : p * 8 + 8, :])
    cosine, sine = cos_sin(ang[0])
    c0[...] = cosine
    s0[...] = sine

    def turn(real, imag, cosine, sine):
        return jnp.concatenate(
            [cosine * real - sine * imag, sine * real + cosine * imag], axis=0
        ).astype(bf16)

    def project(cc):
        first = pl.multiple_of(cc * 2 * SIDES, 2 * SIDES)
        for half in range(2):
            slots = range(half * boxes // 2, (half + 1) * boxes // 2)
            rows = jnp.concatenate(
                [src[inverse[slot], pl.ds(first, 2 * SIDES), :] for slot in slots], axis=0
            )
            prod = jnp.dot(rows, proj[...], preferred_element_type=f32)
            for index, slot in enumerate(slots):
                for part in range(2):
                    at = (index * 2 + part) * SIDES
                    block = prod[at : at + SIDES]
                    sent[cc * 2 + part, slot] = turn(
                        block[:, :coeffs], block[:, coeffs:],
                        c0[slot : slot + 1, :], s0[slot : slot + 1, :],
                    )

    def in_copy(c, j, i):
        x, y, slot = spot(j, i)
        return pltpu.make_async_remote_copy(
            src_ref=sent.at[c, slot], dst_ref=got.at[c, mine],
            send_sem=in_send.at[c], recv_sem=in_recv.at[c],
            device_id=(x, y), device_id_type=pl.DeviceIdType.MESH,
        )

    def phase_copy(j, i):
        x, y, slot = spot(j, i)
        return pltpu.make_async_remote_copy(
            src_ref=phase_out.at[slot], dst_ref=phase_in.at[mine],
            send_sem=ang_send.at[0], recv_sem=ang_recv.at[0],
            device_id=(x, y), device_id_type=pl.DeviceIdType.MESH,
        )

    def last_copy(j):
        p = (me_y + j) % count_y
        return pltpu.make_async_remote_copy(
            src_ref=last_out.at[p], dst_ref=last_in.at[me_y],
            send_sem=ang_send.at[1], recv_sem=ang_recv.at[1],
            device_id=(me_x, p), device_id_type=pl.DeviceIdType.MESH,
        )

    def out_copy(c, odd, k):
        return pltpu.make_async_remote_copy(
            src_ref=back.at[c, odd, onto(k)], dst_ref=home.at[c, odd, group],
            send_sem=out_send.at[c, odd], recv_sem=out_recv.at[c, odd],
            device_id=(group_low + xl * onto(k), me_y), device_id_type=pl.DeviceIdType.MESH,
        )

    far = sorted(range(count_y), key=lambda j: -min(j // 2, count_y // 2 - j // 2))
    blocks = [(j, i) for j in far for i in range(per_peer)]
    early = [(j, i) for j, i in blocks if j < 2]
    late = [(j, i) for j, i in blocks if j >= 2]

    def keep(copy_own):
        if simple:
            copy_own(spot(0, 0)[2])
        else:
            for i in range(per_peer):
                x, _, slot = spot(0, i)
                pl.when(x == me_x)(functools.partial(copy_own, slot))

    def settle(ref, sem, count):
        if simple:
            block = ref.at[pl.ds(0, count)]
            pltpu.make_async_copy(block, block, sem).wait()
        else:
            block = ref.at[pl.ds(0, count - own)]
            pltpu.make_async_copy(block, block, sem).wait()

    total = boxes - 1 if simple else boxes

    def send_part(c, part):
        for j, i in part:
            remote(j, i, lambda: in_copy(c, j, i).start())

    def keep_chunk(c):
        def copy_own(slot):
            got[c, mine] = sent[c, slot]

        keep(copy_own)

    def send_chunk(c):
        send_part(c, late)

    loads[1].wait()
    pieces.wait()
    project(0)

    near = [(j, i) for j, i in blocks if j == 0 or i == 0] if simple else blocks
    others = [(j, i) for j, i in blocks if j and i] if simple else []
    pl.semaphore_wait(barrier, expected)
    if simple:
        for k in range(1, nx):
            pl.semaphore_signal(
                ready, inc=1, device_id=(onto(k), me_y), device_id_type=pl.DeviceIdType.MESH
            )
    for j, i in near:
        remote(j, i, lambda: phase_copy(j, i).start())
    send_part(0, near)
    for j in range(1, count_y):
        last_copy(j).start()
    send_part(1, near)

    def own_phase(slot):
        phase_in[mine] = phase_out[slot]

    keep(own_phase)
    last_in[me_y] = last_out[me_y]
    keep_chunk(0)
    keep_chunk(1)
    if simple:
        pl.semaphore_wait(ready, nx - 1)
    for j, i in others:
        remote(j, i, lambda: phase_copy(j, i).start())
    send_part(0, others)
    send_part(1, others)

    @pl.loop(1, pairs)
    def _(cc):
        project(cc)
        for c in (cc * 2, cc * 2 + 1):
            send_part(c, early)
            keep_chunk(c)

    loads[2].wait()
    loads[3].wait()
    settle(phase_in, ang_recv.at[0], total)
    cosine, sine = cos_sin(decode(phase_in[...]))
    cs[...] = cosine
    sn[...] = sine
    seen = last_in.at[pl.ds(0, count_y - 1)]
    pltpu.make_async_copy(seen, seen, ang_recv.at[1]).wait()
    cosine, sine = cos_sin(decode(last_in[...]))
    cs_last[...] = cosine
    sn_last[...] = sine

    def wide(ref, block, row):
        return jnp.concatenate(
            [ref[block, row : row + 1, :], ref[block, row + 1 : row + 2, :]], axis=1
        )

    def level(load, store, number, stride, phase, odd=(0, 1)):
        lows = [b for b in range(nx * ny) if b // stride % 2 == 0 and b % 2 in odd]
        low = jnp.concatenate([load(b) for b in lows], axis=0)
        high = jnp.concatenate([load(b + stride) for b in lows], axis=0)
        for h in range(2):
            prod = jnp.dot(low, w[number, h, :coeffs, :], preferred_element_type=f32)
            prod += jnp.dot(high, w[number, h, coeffs:, :], preferred_element_type=f32)
            values = []
            for index, b in enumerate(lows):
                base = index * 2 * SIDES
                upper, lower = prod[base : base + SIDES], prod[base + SIDES : base + 2 * SIDES]
                real = upper[:, :coeffs] - lower[:, coeffs:]
                imag = lower[:, :coeffs] + upper[:, coeffs:]
                values.append((b + h * stride, turn(real, imag, *phase(b + h * stride))))
            store(values)

    def into(ref):
        def store(values):
            for b, value in values:
                ref[b] = value

        return store

    def phases(number):
        return lambda b: (wide(cs, b, number * 2), wide(sn, b, number * 2))

    def last_phases(b):
        g, yy = b // ny, b % ny
        y, row = yy * yl + g % yl, g // yl * 2
        return wide(cs_last, y, row), wide(sn_last, y, row)

    def middle(c):
        settle(got.at[c], in_recv.at[c], total)

        @pl.when(c + AHEAD < chunks)
        def _():
            send_chunk(c + AHEAD)


        def store(values):
            for b, value in values:
                back[c, b % 2, b // ny, b % ny // 2] = value

        for odd in range(2):
            level(lambda b: got[c, b], into(ping), 0, 4, phases(0), (odd,))
            level(lambda b: ping[b], into(pong), 1, 2 * ny, phases(1), (odd,))
            level(lambda b: pong[b], into(ping), 2, 2, phases(2), (odd,))
            level(lambda b: ping[b], store, 3, ny, phases(3), (odd,))
            for k in range(1, nx):
                out_copy(c, odd, k).start()
            home[c, odd, group] = back[c, odd, group]

    def final(c):
        for odd in range(2):
            seen = home.at[c, odd, pl.ds(0, nx - 1)]
            pltpu.make_async_copy(seen, seen, out_recv.at[c, odd]).wait()
        first = pl.multiple_of(c * SIDES, SIDES)

        def store(values):
            rows = jnp.concatenate([value for _, value in values], axis=0)
            prod = jnp.dot(rows, interp[...], preferred_element_type=f32)
            for index, (b, _) in enumerate(values):
                g, yy = b // ny, b % ny
                base = index * 2 * SIDES
                upper, lower = prod[base : base + SIDES], prod[base + SIDES : base + 2 * SIDES]
                real = upper[:, :points] - lower[:, points:]
                imag = upper[:, points:] + lower[:, :points]
                slot = (yy * yl + g % yl) * per_peer + g // yl
                out_ref[slot, pl.ds(first, SIDES), :] = real.astype(bf16)
                out_ref[slot, pl.ds(first + sides, SIDES), :] = imag.astype(bf16)

        level(lambda b: home[c, b % 2, b // ny, b % ny // 2], store, 4, 1, last_phases)

    @pl.loop(0, chunks + 1)
    def _(t):
        @pl.when(t < chunks)
        def _():
            middle(t)

        @pl.when(t == chunks)
        def _():
            for c in range(chunks):
                settle(sent.at[c], in_send.at[c], total)
                for odd in range(2):
                    seen = back.at[c, odd, pl.ds(0, nx - 1)]
                    pltpu.make_async_copy(seen, seen, out_send.at[c, odd]).wait()
            settle(phase_out, ang_send.at[0], total)
            seen = last_out.at[pl.ds(0, count_y - 1)]
            pltpu.make_async_copy(seen, seen, ang_send.at[1]).wait()

        @pl.when(t >= 1)
        def _():
            final(t - 1)


def local(sources, projection, translations, angles, interpolation, box_order):
    boxes, sides, points = sources.shape
    coeffs = projection.shape[1] // 2
    count_x, count_y = lax.axis_size("gx"), lax.axis_size("gy")
    chunks = sides // SIDES
    f32, bf16 = jnp.float32, jnp.bfloat16
    anywhere = pl.BlockSpec(memory_space=pltpu.HBM)
    vmem = pl.BlockSpec(memory_space=pltpu.VMEM)
    state = pltpu.VMEM((chunks, boxes, 2 * SIDES, coeffs), bf16)
    one = pltpu.VMEM((boxes, 2 * SIDES, coeffs), bf16)
    grouped = pltpu.VMEM((chunks, 2, 4, boxes // 8, 2 * SIDES, coeffs), bf16)
    lanes = coeffs // 2
    phases, last = pltpu.VMEM((boxes, 8, lanes), f32), pltpu.VMEM((count_y, 8, lanes), f32)
    coded, coded_last = (
        pltpu.VMEM((boxes, 8, lanes), jnp.int16), pltpu.VMEM((count_y, 8, lanes), jnp.int16)
    )
    dma = pltpu.SemaphoreType.DMA
    return pl.pallas_call(
        functools.partial(kernel, count_x, count_y, sides),
        out_shape=pltpu.VMEM((boxes, 2 * sides, points), bf16),
        in_specs=[vmem] + [anywhere] * 5,
        out_specs=vmem,
        scratch_shapes=[
            pltpu.VMEM(angles.shape, f32), pltpu.VMEM(sources.shape, bf16),
            pltpu.VMEM(projection.shape, bf16), pltpu.VMEM(translations.shape, bf16),
            pltpu.VMEM(interpolation.shape, bf16), pltpu.SMEM((boxes,), jnp.int32),
            pltpu.VMEM((boxes, coeffs), f32), pltpu.VMEM((boxes, coeffs), f32),
            state, state, one, one, grouped, grouped,
            pltpu.VMEM((boxes * 8, lanes), f32), pltpu.VMEM((count_y * 8, lanes), f32),
            coded, coded, coded_last, coded_last, phases, phases, last, last,
            pltpu.SemaphoreType.REGULAR, dma((5,)), dma((chunks,)), dma((chunks,)), dma((chunks, 2)),
            dma((chunks, 2)), dma((2,)), dma((2,)),
        ],
        compiler_params=pltpu.CompilerParams(
            collective_id=0, has_side_effects=True, vmem_limit_bytes=40 * 2**20
        ),
    )(
        *[
            pltpu.with_memory_space_constraint(value, pltpu.HBM)
            for value in (
                box_order.reshape(1, boxes), angles, sources, projection, translations,
                interpolation,
            )
        ]
    )


def solution(mesh):
    placed = (
        P(("gx", "gy"), None, None),
        P(),
        P(),
        P(None, ("gx", "gy"), None),
        P(),
        P(("gx", "gy")),
    )
    return jax.shard_map(
        local, mesh=mesh, in_specs=placed, out_specs=P(("gx", "gy"), None, None), check_vma=False
    )
```
